32 devices in a mesh: ep: 4 (over x, core), fsdp: 8 (over z, y).
Axes of the slice: x: 2, y: 2, z: 4, core: 2. Of those that a mesh axis runs over, the one named last changes fastest.
Arguments:
- train_gate: float32 [128, 2048, 768], P('ep', 'fsdp'), may hold values from -0.1875 to 0.1875
- other_gate: bfloat16 [128, 2048, 768], P('ep', 'fsdp'), may hold values from -0.0625 to 0.0625
- train_up: float32 [128, 2048, 768], P('ep', 'fsdp'), may hold values from -0.1875 to 0.1875
- other_up: bfloat16 [128, 2048, 768], P('ep', 'fsdp'), may hold values from -0.0625 to 0.0625
- router_weight: float32 [2048, 128], P('fsdp', 'ep'), may hold values from -0.125 to 0.125
- router_gain: float32 [2048], P('fsdp'), may hold values from 0.25 to 1.75
Outputs:
- ready_gate: bfloat16 [128, 2048, 768], P('ep', None, 'fsdp')
- ready_up: bfloat16 [128, 2048, 768], P('ep', None, 'fsdp')
- scale_gate: float32 [128, 768], P('ep', 'fsdp')
- scale_up: float32 [128, 768], P('ep', 'fsdp')
- serve_router: bfloat16 [2048, 128], replicated
The draws below stay inside these ranges and needn't reach their ends.
All inputs are finite; a program needn't handle non-finite values. Where the reference program divides by a largest or mean magnitude, that divisor is 1e-20 or more.
Results may differ from the reference program's by a relative error of at most 0.001.
Values may be sent and summed in bfloat16 or wider, within the bound.
A program may use at most 256 MiB of HBM per device.

```python
import jax
import jax.numpy as jnp

EXPERTS = 128
D_MODEL = 2048
D_EXPERT = 768


def spiked(values, stream_key, source, target, parts, factor):
    def block_of(axis_at):
        return (jnp.arange(values.shape[axis_at]) // (values.shape[axis_at] // parts)).reshape((-1,) + (1,) * (values.ndim - 1 - axis_at))

    first = jax.random.permutation(stream_key, parts)[block_of(target)]
    second = (block_of(target) + parts // 2) % parts
    return jnp.where((block_of(source) == first) | (block_of(source) == second), factor * values, values)


def level_of(own_key, shape, split, least, top_value):
    def one(position, parts):
        draws = jax.random.uniform(jax.random.fold_in(jax.random.fold_in(own_key, 6), position), (parts,), jnp.float32, least / len(split), top_value / len(split))
        return jnp.repeat(jnp.exp(draws), shape[position] // parts).reshape((-1,) + (1,) * (len(shape) - position - 1))

    gain = one(*split[0])
    for cut in split[1:]:
        gain = gain * one(*cut)
    return gain


def normal_values(key, extent, deviation, bound, cuts=(), held_as=jnp.bfloat16):
    level = level_of(key, extent, cuts, -0.22, 0.18) if cuts else 1.0
    values = jax.random.normal(key, extent, jnp.float32) * deviation * level
    return jnp.minimum(jnp.maximum(values, -bound), bound).astype(held_as)


def noise_with(stream_key, shape, spread, reach, cuts, heavy, held_as=jnp.bfloat16):
    entries = spread * jax.random.normal(stream_key, shape, jnp.float32)
    if cuts:
        entries = entries * level_of(stream_key, shape, cuts, -0.22, 0.18)
    return jnp.clip(spiked(entries, jax.random.fold_in(stream_key, 3), *heavy), -reach, reach).astype(held_as)


def setup_inputs(seed: int = 0) -> dict:
    key_of = jax.random.split(jax.random.key(seed), 7)
    return {
        "train_gate": noise_with(key_of[0], (EXPERTS, D_MODEL, D_EXPERT), D_MODEL ** -0.5, 0.1875, ((0, 4), (1, 8)), (1, 2, 8, 2.0), jnp.float32),
        "other_gate": normal_values(key_of[1], (EXPERTS, D_MODEL, D_EXPERT), (D_MODEL * 4) ** -0.5, 0.0625, ((0, 4), (1, 8))),
        "train_up": noise_with(key_of[2], (EXPERTS, D_MODEL, D_EXPERT), D_MODEL ** -0.5, 0.1875, ((0, 4), (1, 8)), (1, 2, 8, 2.0), jnp.float32),
        "other_up": normal_values(key_of[3], (EXPERTS, D_MODEL, D_EXPERT), (D_MODEL * 4) ** -0.5, 0.0625, ((0, 4), (1, 8))),
        "router_weight": normal_values(key_of[4], (D_MODEL, EXPERTS), D_MODEL ** -0.5, 0.125, ((0, 8), (1, 4)), jnp.float32),
        "router_gain": jnp.clip(1.0 + 0.15 * jax.random.normal(key_of[5], (D_MODEL,), jnp.float32), 0.25, 1.75),
    }


def reference(train_gate, other_gate, train_up, other_up, router_weight, router_gain):
    latest_gate = train_gate + other_gate.astype(jnp.float32)
    latest_up = train_up + other_up.astype(jnp.float32)
    scale_gate = jnp.sum(jnp.abs(latest_gate), axis=1) / D_MODEL
    ready_gate = (latest_gate / jnp.expand_dims(scale_gate, 1)).astype(jnp.bfloat16)
    scale_up = jnp.sum(jnp.abs(latest_up), axis=1) / D_MODEL
    ready_up = (latest_up / jnp.expand_dims(scale_up, 1)).astype(jnp.bfloat16)
    serve_router = (router_weight * router_gain[:, None]).astype(jnp.bfloat16)
    return ready_gate, ready_up, scale_gate, scale_up, serve_router
```

```python
import functools

import jax
import jax.numpy as jnp
from jax import lax
from jax.experimental import pallas as pl
from jax.experimental.pallas import tpu as pltpu
from jax.sharding import PartitionSpec as P

MESH = pl.DeviceIdType.MESH
SLOTS = 3


def plain_device(train_gate, other_gate, train_up, other_up, router_weight, router_gain):
    latest_gate = train_gate + other_gate.astype(jnp.float32)
    latest_up = train_up + other_up.astype(jnp.float32)
    depth = train_gate.shape[1] * lax.axis_size("fsdp")
    total_gate, total_up = lax.psum(
        (jnp.sum(jnp.abs(latest_gate), axis=1), jnp.sum(jnp.abs(latest_up), axis=1)), "fsdp"
    )
    scale_gate = total_gate / depth
    scale_up = total_up / depth
    narrow_gate = (latest_gate / jnp.expand_dims(scale_gate, 1)).astype(jnp.bfloat16)
    narrow_up = (latest_up / jnp.expand_dims(scale_up, 1)).astype(jnp.bfloat16)
    ready_gate = lax.all_to_all(narrow_gate, "fsdp", split_axis=2, concat_axis=1, tiled=True)
    ready_up = lax.all_to_all(narrow_up, "fsdp", split_axis=2, concat_axis=1, tiled=True)
    width = ready_gate.shape[2]
    start = lax.axis_index("fsdp") * width
    scale_gate = lax.dynamic_slice_in_dim(scale_gate, start, width, axis=1)
    scale_up = lax.dynamic_slice_in_dim(scale_up, start, width, axis=1)
    part_router = (router_weight * router_gain[:, None]).astype(jnp.bfloat16)
    row_router = lax.all_gather(part_router, "fsdp", axis=0, tiled=True)
    serve_router = lax.all_gather(row_router, "ep", axis=1, tiled=True)
    return (ready_gate, ready_up, scale_gate, scale_up, serve_router)


def far_first(n):
    return sorted(range(1, n), key=lambda d: (abs(d - n // 2), d))


def kernel(n, p, tg, og, tu, ou, rw, rgain, ready_gate, ready_up, scale_gate, scale_up, router,
           wide, narrow, send, part_a, land_a, tot_a, part_b, land_b, tot_b, rows_r, all_r,
           in_sem, own_sem, send_sem, recv_sem, small_send, small_recv, r_send, r_recv):
    experts, depth, width = tg.shape
    piece = width // n
    me = lax.axis_index("fsdp")
    group = lax.axis_index("ep")
    first = n // 2
    trains, others = (tg, tu), (og, ou)
    readys, scales = (ready_gate, ready_up), (scale_gate, scale_up)
    peers = [(me + d) % n for d in far_first(n)]
    twins = [(group + d) % p for d in range(1, p)]

    barrier = pltpu.get_barrier_semaphore()
    for peer in peers:
        pl.semaphore_signal(barrier, inc=1, device_id={"fsdp": peer}, device_id_type=MESH)
    for twin in twins:
        pl.semaphore_signal(barrier, inc=1, device_id={"ep": twin}, device_id_type=MESH)

    def loads(e, slot):
        return [
            pltpu.make_async_copy(src.at[e], dst.at[m, slot], in_sem.at[k, m, slot])
            for m in range(2)
            for k, (src, dst) in enumerate(((trains[m], wide), (others[m], narrow)))
        ]

    def over(low, high, body):
        for e in range(low, min(low + SLOTS - 1, high)):
            for copy in loads(e, (e - low) % SLOTS):
                copy.start()

        def step(i, _):
            e = low + i
            slot = lax.rem(i, SLOTS)

            @pl.when(e + SLOTS - 1 < high)
            def _():
                for copy in loads(e + SLOTS - 1, lax.rem(i + SLOTS - 1, SLOTS)):
                    copy.start()

            for copy in loads(e, slot):
                copy.wait()
            for m in range(2):
                body(e, m, slot)
            return 0

        lax.fori_loop(0, high - low, step, 0)

    def sums(base, part, share):
        def body(e, m, slot):
            at = (e - base) * 2 + m
            latest = wide[m, slot] + narrow[m, slot].astype(jnp.float32)
            row = jnp.sum(jnp.abs(latest), axis=0, keepdims=True)
            part[at // share, pl.ds(at % share, 1), :] = row

        return body

    def ready(base, tot, share):
        def body(e, m, slot):
            at = (e - base) * 2 + m
            scale = tot[at // share, pl.ds(at % share, 1), :] / (n * depth)
            scales[m][pl.ds(e, 1), :] = scale
            inverse = 1.0 / scale
            step = 128
            for c in range(0, width, step):
                latest = wide[m, slot, :, c:c + step] + narrow[m, slot, :, c:c + step].astype(jnp.float32)
                value = latest * inverse[:, c:c + step]
                send[m, e, c:c + step, :] = value.T.astype(jnp.bfloat16)
            place = readys[m].at[e, :, pl.ds(pl.multiple_of(me * depth, 128), depth)]
            for peer in peers:
                pltpu.make_async_remote_copy(
                    src_ref=send.at[m, e, pl.ds(pl.multiple_of(peer * piece, 16), piece), :],
                    dst_ref=place,
                    send_sem=send_sem.at[m],
                    recv_sem=recv_sem.at[m],
                    device_id={"fsdp": peer},
                    device_id_type=MESH,
                ).start()
            pltpu.make_async_copy(
                send.at[m, e, pl.ds(pl.multiple_of(me * piece, 16), piece), :], place, own_sem.at[m]
            ).start()

        return body

    def push(src, dst, at, axis, targets, s, r):
        for target, block in zip(targets, src):
            pltpu.make_async_remote_copy(
                src_ref=block, dst_ref=dst.at[at], send_sem=s, recv_sem=r,
                device_id={axis: target}, device_id_type=MESH,
            ).start()

    def drain(ref, sem):
        pltpu.make_async_copy(ref, ref, sem).wait()

    def scatter(part, land, k):
        push([part.at[peer] for peer in peers], land, me, "fsdp", peers, small_send.at[k], small_recv.at[k])
        land[me] = part[me]

    def gather(land, tot, k):
        drain(land.at[pl.ds(0, n - 1)], small_recv.at[k])
        tot[me] = jnp.sum(land[...], axis=0)
        push([tot.at[me]] * (n - 1), tot, me, "fsdp", peers, small_send.at[k + 1], small_recv.at[k + 1])

    def gathered(tot, k):
        drain(tot.at[pl.ds(0, n - 1)], small_recv.at[k + 1])

    share_b = part_b.shape[1]
    over(0, first, sums(0, part_a, 1))
    rows_r[me] = (rw[...] * rgain[...]).astype(jnp.bfloat16)
    pl.semaphore_wait(barrier, n - 1 + p - 1)
    scatter(part_a, land_a, 0)
    gather(land_a, tot_a, 0)
    gathered(tot_a, 0)
    cut = max(first // 2, 1)
    over(0, cut, ready(0, tot_a, 1))
    over(first, experts, sums(first, part_b, share_b))
    scatter(part_b, land_b, 2)
    push([rows_r.at[me]] * (n - 1), rows_r, me, "fsdp", peers, r_send.at[0], r_recv.at[0])
    middle = (cut + first) // 2
    over(cut, middle, ready(0, tot_a, 1))
    gather(land_b, tot_b, 2)
    over(middle, first, ready(0, tot_a, 1))
    gathered(tot_b, 2)
    later = first + (experts - first) // 4
    over(first, later, ready(first, tot_b, share_b))
    drain(rows_r.at[pl.ds(0, n - 1)], r_recv.at[0])
    push([rows_r] * (p - 1), all_r, group, "ep", twins, r_send.at[1], r_recv.at[1])
    all_r[group] = rows_r[...]
    over(later, experts, ready(first, tot_b, share_b))
    if p > 1:
        drain(all_r.at[pl.ds(0, p - 1)], r_recv.at[1])
    for f in range(n):
        block = all_r[:, f].astype(jnp.float32)
        block = block.reshape(block.shape[0] * block.shape[1], depth)
        router[f * depth:(f + 1) * depth, :] = block.T.astype(jnp.bfloat16)
    for k, (part, tot) in enumerate(((part_a, tot_a), (part_b, tot_b))):
        drain(part.at[pl.ds(0, n - 1)], small_send.at[2 * k])
        drain(tot.at[pl.ds(0, n - 1)], small_send.at[2 * k + 1])
    drain(rows_r.at[pl.ds(0, n - 1)], r_send.at[0])
    if p > 1:
        drain(all_r.at[pl.ds(0, p - 1)], r_send.at[1])
    for m in range(2):
        drain(send.at[m, :, pl.ds(0, piece), :], own_sem.at[m])
        drain(send.at[m, :, pl.ds(0, width - piece), :], send_sem.at[m])
        drain(readys[m].at[:, :, pl.ds(0, (n - 1) * depth)], recv_sem.at[m])


def sending_device(n, p, train_gate, other_gate, train_up, other_up, router_weight, router_gain):
    experts, depth, width = train_gate.shape
    piece = width // n
    columns = router_weight.shape[1]
    share = (2 * experts - n) // n
    f32, bf16 = jnp.float32, jnp.bfloat16
    anywhere = pl.BlockSpec(memory_space=pl.ANY)
    vmem = pl.BlockSpec(memory_space=pltpu.VMEM)
    ready = jax.ShapeDtypeStruct((experts, piece, n * depth), bf16)
    scale = jax.ShapeDtypeStruct((experts, width), f32)
    stats = [pltpu.VMEM((n, 1, width), f32)] * 3 + [pltpu.VMEM((n, share, width), f32)] * 3
    dma = pltpu.SemaphoreType.DMA
    ready_gate, ready_up, scale_gate, scale_up, router = pl.pallas_call(
        functools.partial(kernel, n, p),
        out_shape=(ready, ready, scale, scale, jax.ShapeDtypeStruct((n * depth, p * columns), bf16)),
        in_specs=[anywhere] * 4 + [vmem] * 2,
        out_specs=(anywhere, anywhere, vmem, vmem, vmem),
        scratch_shapes=[
            pltpu.VMEM((2, SLOTS, depth, width), f32),
            pltpu.VMEM((2, SLOTS, depth, width), bf16),
            pltpu.VMEM((2, experts, width, depth), bf16),
            *stats,
            pltpu.VMEM((n, columns, depth), bf16),
            pltpu.VMEM((p, n, columns, depth), bf16),
            dma((2, 2, SLOTS)), dma((2,)), dma((2,)), dma((2,)), dma((4,)), dma((4,)), dma((2,)), dma((2,)),
        ],
        compiler_params=pltpu.CompilerParams(
            collective_id=0, has_side_effects=True, vmem_limit_bytes=60 * 2**20
        ),
        name="send_ready",
    )(train_gate, other_gate, train_up, other_up, router_weight.T, router_gain[None, :])
    start = lax.axis_index("fsdp") * piece
    return (
        jnp.swapaxes(ready_gate, 1, 2),
        jnp.swapaxes(ready_up, 1, 2),
        lax.dynamic_slice_in_dim(scale_gate, start, piece, axis=1),
        lax.dynamic_slice_in_dim(scale_up, start, piece, axis=1),
        router,
    )


def solution(mesh):
    n, p = mesh.shape["fsdp"], mesh.shape["ep"]

    def per_device(*args):
        experts, depth, width = args[0].shape
        fits = (
            depth % 128 == 0 and width % (16 * n) == 0 and width % 128 == 0 and n % 2 == 0
            and 2 * experts % n == 0 and 2 * experts > n and args[4].shape[1] % 16 == 0
            and 2 * experts * depth * width * 2 <= 2**25
        )
        return sending_device(n, p, *args) if fits else plain_device(*args)

    matrix = P("ep", "fsdp", None)
    in_specs = (matrix, matrix, matrix, matrix, P("fsdp", "ep"), P("fsdp"))
    out_specs = (P("ep", None, "fsdp"), P("ep", None, "fsdp"), P("ep", "fsdp"), P("ep", "fsdp"), P())
    return jax.shard_map(
        per_device, mesh=mesh, in_specs=in_specs, out_specs=out_specs, check_vma=False
    )
```
